256 devices in a mesh: groups: 2 (over y), seq: 128 (over z, x, core).
Axes of the slice: x: 4, y: 2, z: 16, core: 2. Of those that a mesh axis runs over, the one named last changes fastest.
The devices are a block of a 4x16x16 slice.
Arguments:
- query_rows: bfloat16 [16384, 2048], P(('groups', 'seq')), parts along dimension 0, may hold values from -180 to 180
- key_rows: bfloat16 [16384, 512], P(('groups', 'seq')), parts along dimension 0, may hold values from -6 to 6
- value_rows: bfloat16 [16384, 512], P(('groups', 'seq')), parts along dimension 0, may hold values from -6 to 6
- positions: int32 [16384], P(('groups', 'seq')), parts along dimension 0, may hold values from 0 to 8191, as said below
- prompt_length: int32 [2], P('groups'), parts along dimension 0, may hold values from 4096 to 8192
- out_weight: bfloat16 [2048, 2048], replicated, may hold values from -0.125 to 0.125
- residual: bfloat16 [16384, 2048], P(('groups', 'seq')), parts along dimension 0, may hold values from -0.59765625 to 0.59765625
Outputs:
- layer_out: bfloat16 [16384, 2048], P(('groups', 'seq')), parts along dimension 0
The draws below stay inside these ranges and needn't reach their ends.
There are 2 independent parts, one for each index of `groups`. The reference program is written for one: setup_inputs(seed, part) draws one part's arguments, and reference() takes and returns one part's arrays. A program takes and returns all parts, laid end to end along the dimension named above; an argument that names none is the same for every part. Nothing has to cross between parts.
Inputs may be any that keep to these rules, and one draw needn't show every extreme that they name: A permutation of 0 to 8191 in which each device's rows hold exactly one position of every run of 128 consecutive positions.
All inputs are finite; a program needn't handle non-finite values.
Results may differ from the reference program's by a relative error of at most 0.009.
Values may be sent and summed in bfloat16 or wider, within the bound.
No kernel may reach another device: no remote copies, remote signals or barrier semaphores. Data moves between devices by JAX's collectives and lax.ppermute only.
A program may use at most 128 MiB of HBM per device.

```python
import math
import jax
import jax.numpy as jnp
from jax import lax

HEADS = 16
KV_HEADS = 4
HEAD_DIM = 128
OUT_FEAT = 2048
TOK_DEV = 64
ATTN = 2048
LEN = 8192
N_SEQ = 128


def pair_draw(key):
    base = jax.random.fold_in(key, 41)
    seed_query, seed_key = jax.random.split(base, 2)
    group_size = HEADS // KV_HEADS
    key_vals = jnp.clip(jax.random.normal(seed_key, (LEN, KV_HEADS, HEAD_DIM), jnp.float32), -6.0, 6.0)
    query_vals = jnp.clip(jax.random.normal(seed_query, (LEN, KV_HEADS, group_size, HEAD_DIM), jnp.float32), -6.0, 6.0)
    return (query_vals.reshape(LEN, HEADS * HEAD_DIM), key_vals.reshape(LEN, KV_HEADS * HEAD_DIM))


def draw_query_rows(key, part):
    return pair_draw(key)[0].astype(jnp.bfloat16)


def draw_key_rows(key, part):
    return pair_draw(key)[1].astype(jnp.bfloat16)


def draw_positions(key, part):
    device_order = jax.random.permutation(jax.random.fold_in(key, 5), N_SEQ)
    row_index = jnp.arange(LEN, dtype=jnp.int32)
    return (row_index % TOK_DEV * N_SEQ + device_order[row_index // TOK_DEV]).astype(jnp.int32)


def block_levels(rng, dims, shards, least, high):
    def one(axis_at, shards_of):
        heights = jax.random.uniform(jax.random.fold_in(jax.random.fold_in(rng, 6), axis_at), (shards_of,), jnp.float32, least / len(shards), high / len(shards))
        return jnp.repeat(jnp.exp(heights), dims[axis_at] // shards_of).reshape((-1,) + (1,) * (len(dims) - axis_at - 1))

    factor_of = one(*shards[0])
    for cut in shards[1:]:
        factor_of = factor_of * one(*cut)
    return factor_of


def bell_draw(stream_key, extent, width, limit, cuts=(), held_as=jnp.bfloat16):
    entries = jax.random.normal(stream_key, extent, jnp.float32) * width
    if len(cuts) > 0:
        entries = block_levels(stream_key, extent, cuts, -0.22, 0.18) * entries
    return jnp.clip(entries, min=-limit, max=limit).astype(held_as)


def setup_inputs(seed: int = 0, part: int = 0) -> dict:
    key_of = jax.random.split(jax.random.key(seed), 8)
    part_splits = jax.random.split(jax.random.fold_in(key_of[7], part), 8)
    return {
        "query_rows": draw_query_rows(jax.random.fold_in(jax.random.fold_in(key_of[7], part), 71), part),
        "key_rows": draw_key_rows(jax.random.fold_in(jax.random.fold_in(key_of[7], part), 71), part),
        "value_rows": bell_draw(part_splits[2], (LEN, KV_HEADS * HEAD_DIM), 1.0, 6.0, ((0, 128),)),
        "positions": draw_positions(jax.random.fold_in(jax.random.fold_in(key_of[7], part), 71), part),
        "prompt_length": jax.random.randint(part_splits[4], (1,), LEN // 2, LEN + 1).astype(jnp.int32),
        "out_weight": bell_draw(key_of[5], (ATTN, OUT_FEAT), ATTN ** -0.5, 0.125),
        "residual": bell_draw(part_splits[6], (LEN, OUT_FEAT), 0.1, 0.59765625, ((0, 128),)),
    }


def reference(query_rows, key_rows, value_rows, positions, prompt_length, out_weight, residual):
    group_size = HEADS // KV_HEADS
    key_all = key_rows.reshape(LEN, KV_HEADS, HEAD_DIM).astype(jnp.float32)
    value_all = value_rows.reshape(LEN, KV_HEADS, HEAD_DIM).astype(jnp.float32)
    prompt_limit = prompt_length[0]
    block_rows = math.gcd(LEN, 512)
    block_count = LEN // block_rows
    query_blocks = query_rows.reshape(block_count, block_rows, KV_HEADS, group_size, HEAD_DIM)
    position_blocks = positions.reshape(block_count, block_rows)

    def attend(inputs):
        query_part, query_pos = inputs
        scores = jnp.einsum("qhgd,khd->hgqk", query_part.astype(jnp.float32), key_all) * HEAD_DIM ** -0.5
        visible = (positions[None, :] <= query_pos[:, None]) & (positions[None, :] < prompt_limit)
        scores = jnp.where(visible[None, None], scores, -1e30)
        maxima = jnp.max(scores, axis=-1, keepdims=True)
        weights = jnp.where(visible[None, None], jnp.exp(scores - maxima), 0.0)
        totals = jnp.sum(weights, axis=-1)
        rounded = lax.optimization_barrier(weights.astype(jnp.bfloat16))
        numerators = jnp.einsum("hgqk,khd->hgqd", rounded.astype(jnp.float32), value_all)
        attended = numerators / totals[..., None]
        return attended.transpose(2, 0, 1, 3).reshape(block_rows, HEADS * HEAD_DIM).astype(jnp.bfloat16)

    attended = lax.map(attend, (query_blocks, position_blocks)).reshape(LEN, HEADS * HEAD_DIM)
    projected = jnp.dot(attended, out_weight, preferred_element_type=jnp.float32)
    return (projected + residual.astype(jnp.float32)).astype(jnp.bfloat16)
```

```python
import functools
import math
import jax
import jax.numpy as jnp
from jax import lax
from jax.experimental import pallas as pl
from jax.experimental.pallas import tpu as pltpu
from jax.sharding import PartitionSpec as P

HEADS = 16
KV_HEADS = 4
HEAD_DIM = 128
GROUP = HEADS // KV_HEADS
TOK = 64
RUN = 128
X_DEV = 4
CORES = 2
BLOCK = KV_HEADS
HALF = 32
KV_ROWS = 2 * TOK + 8
ROWS = 256
SCALE = HEAD_DIM ** -0.5 * math.log2(math.e)
NEVER = -1e30
LOWEST = -1e20
VMEM = pltpu.VMEM
F32 = jnp.float32
BF16 = jnp.bfloat16


def iota(shape, dim):
    return lax.broadcasted_iota(jnp.int32, shape, dim)


def prep_kernel(pos_ref, q_ref, k_ref, v_ref, qs_ref, kv_ref):
    pos = pos_ref[...]
    run = pos // RUN
    off = (pos - run * RUN).astype(F32)
    pick = (iota((TOK, TOK), 0) == jnp.broadcast_to(run, (TOK, TOK))).astype(F32)
    pick16 = pick.astype(BF16)
    off_col = jnp.dot(
        (pick * jnp.broadcast_to(off, (TOK, TOK))).astype(BF16),
        jnp.ones((TOK, HEAD_DIM), BF16),
        preferred_element_type=F32,
    )
    row = iota((TOK, HEAD_DIM), 0)
    lane = iota((TOK, HEAD_DIM), 1)
    lines = [
        jnp.sum(jnp.where(row == HALF * j + lane % HALF, off_col, 0.0), axis=0, keepdims=True)
        for j in range(TOK // HALF)
    ]
    table = jnp.concatenate(lines + [jnp.zeros((8 - len(lines), HEAD_DIM), F32)], axis=0).astype(BF16)
    sorted_q = jnp.dot(pick16, q_ref[...], preferred_element_type=F32).astype(BF16)
    sorted_k = jnp.dot(pick16, k_ref[...], preferred_element_type=F32).astype(BF16)
    sorted_v = jnp.dot(pick16, v_ref[...], preferred_element_type=F32).astype(BF16)
    off16 = off_col.astype(BF16)
    for h in range(KV_HEADS):
        cols = slice(h * HEAD_DIM, (h + 1) * HEAD_DIM)
        kv_ref[h, 0:TOK, :] = sorted_k[:, cols]
        kv_ref[h, TOK:2 * TOK, :] = sorted_v[:, cols]
        kv_ref[h, 2 * TOK:KV_ROWS, :] = table
        for g in range(GROUP):
            at = (h * GROUP + g) * HEAD_DIM
            qs_ref[h, g] = sorted_q[:, at:at + HEAD_DIM]
        qs_ref[h, GROUP] = off16


def prep(positions, query_rows, key_rows, value_rows):
    return pl.pallas_call(
        prep_kernel,
        out_shape=(
            jax.ShapeDtypeStruct((KV_HEADS, GROUP + 1, TOK, HEAD_DIM), BF16),
            jax.ShapeDtypeStruct((KV_HEADS, KV_ROWS, HEAD_DIM), BF16),
        ),
        in_specs=[pl.BlockSpec(memory_space=VMEM)] * 4,
        out_specs=(pl.BlockSpec(memory_space=VMEM),) * 2,
        compiler_params=pltpu.CompilerParams(vmem_limit_bytes=8 * 1024 * 1024),
        cost_estimate=pl.CostEstimate(flops=TOK * TOK * 3072 * 2, bytes_accessed=800_000, transcendentals=0),
        name="prep",
    )(positions.reshape(1, TOK), query_rows, key_rows, value_rows)


def attend_kernel(shards, first, last, *refs):
    limit_ref, qa_ref, qb_ref = refs[:3]
    kv_refs = refs[3:3 + shards]
    refs = refs[3 + shards:]
    if first:
        old_refs = None
    else:
        old_refs, refs = refs[:4], refs[4:]
    new_refs, (keys, vals) = refs[:-2], refs[-2:]
    limit = limit_ref[0]
    wide = shards * HEAD_DIM
    sources = KV_HEADS
    for j in range(2):
        for n, kv in enumerate(kv_refs):
            for s in range(sources):
                at = j * wide + (n * sources + s) * HALF
                keys[at:at + HALF, :] = kv[s, HALF * j:HALF * (j + 1), :]
                vals[at:at + HALF, 0:HEAD_DIM] = kv[s, TOK + HALF * j:TOK + HALF * (j + 1), :]
    vals[:, HEAD_DIM:] = jnp.ones((2 * wide, HEAD_DIM), BF16)
    lane8 = iota((8, HEAD_DIM), 1)
    tables = []
    for kv in kv_refs:
        table = kv[0, 2 * TOK:KV_ROWS, :].astype(F32)
        for s in range(1, sources):
            table = jnp.where(lane8 // HALF == s, kv[s, 2 * TOK:KV_ROWS, :].astype(F32), table)
        table = table + (lane8 % HALF * RUN).astype(F32)
        chunk = (iota((8, HEAD_DIM), 0) * (HALF * RUN)).astype(F32)
        tables.append(jnp.where(table + chunk >= limit.astype(F32), 1e9, table))
    ramp = (iota((HALF, HEAD_DIM), 0) * RUN).astype(F32)
    for half, q_ref in enumerate((qa_ref, qb_ref)):
        for i in range(2):
            for sp in range(2):
                b = i * 2 + sp
                rows_at = slice(HALF * i, HALF * (i + 1))
                q = q_ref[2 * sp:2 * sp + 2, 0:GROUP, rows_at, :].reshape(ROWS, HEAD_DIM)
                q_off = q_ref[2 * sp:2 * sp + 2, GROUP:GROUP + 1, rows_at, :].astype(F32)
                q_pos = jnp.broadcast_to(q_off + ramp[None, None], (2, GROUP, HALF, HEAD_DIM)).reshape(ROWS, HEAD_DIM)
                count = (i + 1) * wide
                s = lax.dot_general(
                    q, keys[0:count, :], (((1,), (1,)), ((), ())), preferred_element_type=F32
                ) * SCALE
                pieces = [s[:, c * HEAD_DIM:(c + 1) * HEAD_DIM] for c in range(count // HEAD_DIM)]
                for n in range(shards):
                    c = i * shards + n
                    pieces[c] = jnp.where(tables[n][i:i + 1, :] <= q_pos, pieces[c], NEVER)
                top = functools.reduce(jnp.maximum, pieces)
                top = jnp.max(top, axis=1, keepdims=True)
                if first:
                    new_max = jnp.broadcast_to(jnp.maximum(top, LOWEST), (ROWS, HEAD_DIM))
                else:
                    old_max = old_refs[2 * half][b]
                    new_max = jnp.maximum(old_max, top)
                weights = jnp.concatenate([jnp.exp2(piece - new_max).astype(BF16) for piece in pieces], axis=1)
                sums = jnp.dot(weights, vals[0:count, :], preferred_element_type=F32)
                if not first:
                    rescale = jnp.exp2(old_max - new_max)
                    sums = sums + old_refs[2 * half + 1][b] * jnp.concatenate([rescale, rescale], axis=1)
                if last and half == 1:
                    lane = iota((ROWS, HEAD_DIM), 1)
                    new_refs[2][b, :, 0:HEAD_DIM] = sums[:, 0:HEAD_DIM]
                    new_refs[2][b, :, HEAD_DIM:] = jnp.where(lane < HEAD_DIM // 2, new_max, sums[:, HEAD_DIM:])
                else:
                    new_refs[2 * half][b] = new_max
                    new_refs[2 * half + 1][b] = sums


def attend(limit, qa, qb, parts, state, last=False):
    shards = len(parts)
    wide = shards * HEAD_DIM
    stats = jax.ShapeDtypeStruct((4, ROWS, HEAD_DIM), F32)
    sums = jax.ShapeDtypeStruct((4, ROWS, 2 * HEAD_DIM), F32)
    shapes = (stats, sums, sums) if last else (stats, sums, stats, sums)
    first = state is None
    held = [] if first else list(state)
    score_count = 4 * 2 * ROWS * 3 * wide
    base = 3 + shards
    return pl.pallas_call(
        functools.partial(attend_kernel, shards, first, last),
        out_shape=shapes,
        in_specs=[pl.BlockSpec(memory_space=pltpu.SMEM)] + [pl.BlockSpec(memory_space=VMEM)] * (2 + shards + len(held)),
        out_specs=(pl.BlockSpec(memory_space=VMEM),) * len(shapes),
        scratch_shapes=[VMEM((2 * wide, HEAD_DIM), BF16), VMEM((2 * wide, 2 * HEAD_DIM), BF16)],
        input_output_aliases={} if first else ({base: 0, base + 1: 1, base + 3: 2} if last else {base + n: n for n in range(4)}),
        compiler_params=pltpu.CompilerParams(vmem_limit_bytes=24 * 1024 * 1024),
        cost_estimate=pl.CostEstimate(
            flops=score_count * HEAD_DIM * 6, bytes_accessed=4_000_000, transcendentals=score_count
        ),
        name="attend_last" if last else "attend",
    )(limit, qa, qb, *parts, *held)


def merge_kernel(max_ref, sum_ref, got_ref, out_ref):
    for i in range(2):
        for sp in range(2):
            b = i * 2 + sp
            max_a = max_ref[b]
            max_b = jnp.broadcast_to(got_ref[b, :, HEAD_DIM:HEAD_DIM + 1], (ROWS, HEAD_DIM))
            total_b = jnp.broadcast_to(got_ref[b, :, 2 * HEAD_DIM - 1:], (ROWS, HEAD_DIM))
            top = jnp.maximum(max_a, max_b)
            part_a = jnp.exp2(max_a - top)
            part_b = jnp.exp2(max_b - top)
            total = sum_ref[b, :, HEAD_DIM:] * part_a + total_b * part_b
            value = sum_ref[b, :, 0:HEAD_DIM] * part_a + got_ref[b, :, 0:HEAD_DIM] * part_b
            value = (value / total).astype(BF16).reshape(2, GROUP, HALF, HEAD_DIM)
            out_ref[2 * sp:2 * sp + 2, :, HALF * i:HALF * (i + 1), :] = value


def merge(maxima, sums, got):
    return pl.pallas_call(
        merge_kernel,
        out_shape=jax.ShapeDtypeStruct((KV_HEADS, GROUP, TOK, HEAD_DIM), BF16),
        in_specs=[pl.BlockSpec(memory_space=VMEM)] * 3,
        out_specs=pl.BlockSpec(memory_space=VMEM),
        compiler_params=pltpu.CompilerParams(vmem_limit_bytes=12 * 1024 * 1024),
        cost_estimate=pl.CostEstimate(flops=4_000_000, bytes_accessed=3_000_000, transcendentals=300_000),
        name="merge",
    )(maxima, sums, got)


def project_kernel(member_ref, pos_ref, *refs):
    parts = refs[:KV_HEADS]
    weight_ref, residual_ref, out_ref, heads = refs[KV_HEADS:]
    member = member_ref[0]
    for d, part in enumerate(parts):
        heads[lax.rem(member + d, KV_HEADS)] = part[...]
    run = pos_ref[...] // RUN
    put = (jnp.broadcast_to(run, (TOK, TOK)) == iota((TOK, TOK), 1)).astype(F32).astype(BF16)
    rows = jnp.concatenate([heads[h, g] for h in range(KV_HEADS) for g in range(GROUP)], axis=1)
    rows = jnp.dot(put, rows, preferred_element_type=F32).astype(BF16)
    wide = 512
    for n in range(weight_ref.shape[1] // wide):
        cols = slice(n * wide, (n + 1) * wide)
        total = jnp.dot(rows, weight_ref[:, cols], preferred_element_type=F32)
        out_ref[:, cols] = (total + residual_ref[:, cols].astype(F32)).astype(BF16)


def project(member, positions, parts, out_weight, residual):
    return pl.pallas_call(
        project_kernel,
        out_shape=jax.ShapeDtypeStruct(residual.shape, BF16),
        in_specs=[pl.BlockSpec(memory_space=pltpu.SMEM)] + [pl.BlockSpec(memory_space=VMEM)] * (len(parts) + 3),
        out_specs=pl.BlockSpec(memory_space=VMEM),
        scratch_shapes=[VMEM((KV_HEADS, GROUP, TOK, HEAD_DIM), BF16)],
        compiler_params=pltpu.CompilerParams(vmem_limit_bytes=20 * 1024 * 1024),
        cost_estimate=pl.CostEstimate(flops=TOK * 2048 * 4096, bytes_accessed=9_000_000, transcendentals=0),
        name="project",
    )(member, positions.reshape(TOK, 1), *parts, out_weight, residual)


def on_device(seq_size, query_rows, key_rows, value_rows, positions, prompt_length, out_weight, residual):
    z_dev = seq_size // (X_DEV * CORES)

    def at(z, x, c):
        return ((z % z_dev) * X_DEV + x % X_DEV) * CORES + c % CORES

    spots = [(z, x, c) for z in range(z_dev) for x in range(X_DEV) for c in range(CORES)]

    def move(a, dz=0, dx=0, dc=0):
        return lax.ppermute(a, "seq", [(at(z, x, c), at(z + dz, x + dx, c + dc)) for z, x, c in spots])

    def turn(a, d):
        return lax.ppermute(
            a, "seq", [(at(z, x, c), at(z // BLOCK * BLOCK + (z + d) % BLOCK, x, c)) for z, x, c in spots]
        )

    member = lax.rem(lax.axis_index("seq") // (X_DEV * CORES), BLOCK)

    def exchange(a):
        pick = [lax.dynamic_index_in_dim(a, lax.rem(member + d, BLOCK), 0, keepdims=False) for d in range(BLOCK)]
        return [pick[0]] + [turn(pick[d], d) for d in range(1, BLOCK)]

    qs, kvs = prep(positions, query_rows, key_rows, value_rows)
    own = jnp.stack(exchange(kvs))
    qa = jnp.stack(exchange(qs))

    def spread(a):
        return [a, move(a, dx=1), move(a, dx=-1), move(a, dx=2)]

    far = [move(own, dz=BLOCK), move(own, dz=-BLOCK), move(own, dz=2 * BLOCK)]
    qb = move(qa, dc=1)
    groups = [spread(own)] + [spread(a) for a in far]
    groups = groups[:3] + [groups[3][:2], groups[3][2:]]
    state = None
    for n, group in enumerate(groups):
        state = attend(prompt_length, qa, qb, group, state, last=n == len(groups) - 1)
    got = move(state[2], dc=1)
    done = merge(state[0], state[1], got)
    parts = [done[0]] + [turn(done[d], -d) for d in range(1, BLOCK)]
    return project(member.reshape(1), positions, parts, out_weight, residual)


def solution(mesh):
    return jax.shard_map(
        functools.partial(on_device, mesh.shape["seq"]),
        mesh=mesh,
        in_specs=(
            P(("groups", "seq"), None),
            P(("groups", "seq"), None),
            P(("groups", "seq"), None),
            P(("groups", "seq")),
            P("groups"),
            P(),
            P(("groups", "seq"), None),
        ),
        out_specs=P(("groups", "seq"), None),
        check_vma=False,
    )
```

```python
import functools
import math
import jax
import jax.numpy as jnp
from jax import lax
from jax.experimental import pallas as pl
from jax.experimental.pallas import tpu as pltpu
from jax.sharding import PartitionSpec as P

HEADS = 16
KV_HEADS = 4
HEAD_DIM = 128
GROUP = HEADS // KV_HEADS
TOK = 64
RUN = 128
X_DEV = 4
CORES = 2
BLOCK = KV_HEADS
HALF = 32
KV_ROWS = 2 * TOK + 8
ROWS = 256
SCALE = HEAD_DIM ** -0.5 * math.log2(math.e)
NEVER = -1e30
LOWEST = -1e20
VMEM = pltpu.VMEM
F32 = jnp.float32
BF16 = jnp.bfloat16


def iota(shape, dim):
    return lax.broadcasted_iota(jnp.int32, shape, dim)


def prep_kernel(pos_ref, q_ref, k_ref, v_ref, qs_ref, kv_ref):
    pos = pos_ref[...]
    run = pos // RUN
    off = (pos - run * RUN).astype(F32)
    pick = (iota((TOK, TOK), 0) == jnp.broadcast_to(run, (TOK, TOK))).astype(F32)
    pick16 = pick.astype(BF16)
    off_col = jnp.dot(
        (pick * jnp.broadcast_to(off, (TOK, TOK))).astype(BF16),
        jnp.ones((TOK, HEAD_DIM), BF16),
        preferred_element_type=F32,
    )
    row = iota((TOK, HEAD_DIM), 0)
    lane = iota((TOK, HEAD_DIM), 1)
    lines = [
        jnp.sum(jnp.where(row == HALF * j + lane % HALF, off_col, 0.0), axis=0, keepdims=True)
        for j in range(TOK // HALF)
    ]
    table = jnp.concatenate(lines + [jnp.zeros((8 - len(lines), HEAD_DIM), F32)], axis=0).astype(BF16)
    sorted_q = jnp.dot(pick16, q_ref[...], preferred_element_type=F32).astype(BF16)
    sorted_k = jnp.dot(pick16, k_ref[...], preferred_element_type=F32).astype(BF16)
    sorted_v = jnp.dot(pick16, v_ref[...], preferred_element_type=F32).astype(BF16)
    off16 = off_col.astype(BF16)
    for h in range(KV_HEADS):
        cols = slice(h * HEAD_DIM, (h + 1) * HEAD_DIM)
        kv_ref[h, 0:TOK, :] = sorted_k[:, cols]
        kv_ref[h, TOK:2 * TOK, :] = sorted_v[:, cols]
        kv_ref[h, 2 * TOK:KV_ROWS, :] = table
        for g in range(GROUP):
            at = (h * GROUP + g) * HEAD_DIM
            qs_ref[h, g] = sorted_q[:, at:at + HEAD_DIM]
        qs_ref[h, GROUP] = off16


def prep(positions, query_rows, key_rows, value_rows):
    return pl.pallas_call(
        prep_kernel,
        out_shape=(
            jax.ShapeDtypeStruct((KV_HEADS, GROUP + 1, TOK, HEAD_DIM), BF16),
            jax.ShapeDtypeStruct((KV_HEADS, KV_ROWS, HEAD_DIM), BF16),
        ),
        in_specs=[pl.BlockSpec(memory_space=VMEM)] * 4,
        out_specs=(pl.BlockSpec(memory_space=VMEM),) * 2,
        compiler_params=pltpu.CompilerParams(vmem_limit_bytes=60 * 1024 * 1024),
        cost_estimate=pl.CostEstimate(flops=TOK * TOK * 3072 * 2, bytes_accessed=800_000, transcendentals=0),
        name="prep",
    )(positions.reshape(1, TOK), query_rows, key_rows, value_rows)


def attend_kernel(shards, first, last, *refs):
    limit_ref, qa_ref, qb_ref = refs[:3]
    kv_refs = refs[3:3 + shards]
    refs = refs[3 + shards:]
    if first:
        old_refs = None
    else:
        old_refs, refs = refs[:4], refs[4:]
    new_refs, (keys, vals) = refs[:-2], refs[-2:]
    limit = limit_ref[0]
    wide = shards * HEAD_DIM
    sources = KV_HEADS
    for j in range(2):
        for n, kv in enumerate(kv_refs):
            for s in range(sources):
                at = j * wide + (n * sources + s) * HALF
                keys[at:at + HALF, :] = kv[s, HALF * j:HALF * (j + 1), :]
                vals[at:at + HALF, 0:HEAD_DIM] = kv[s, TOK + HALF * j:TOK + HALF * (j + 1), :]
    vals[:, HEAD_DIM:] = jnp.ones((2 * wide, HEAD_DIM), BF16)
    lane8 = iota((8, HEAD_DIM), 1)
    tables = []
    for kv in kv_refs:
        table = kv[0, 2 * TOK:KV_ROWS, :].astype(F32)
        for s in range(1, sources):
            table = jnp.where(lane8 // HALF == s, kv[s, 2 * TOK:KV_ROWS, :].astype(F32), table)
        table = table + (lane8 % HALF * RUN).astype(F32)
        chunk = (iota((8, HEAD_DIM), 0) * (HALF * RUN)).astype(F32)
        tables.append(jnp.where(table + chunk >= limit.astype(F32), 1e9, table))
    ramp = (iota((HALF, HEAD_DIM), 0) * RUN).astype(F32)
    for half, q_ref in enumerate((qa_ref, qb_ref)):
        for i in range(2):
            for sp in range(2):
                b = i * 2 + sp
                rows_at = slice(HALF * i, HALF * (i + 1))
                q = q_ref[2 * sp:2 * sp + 2, 0:GROUP, rows_at, :].reshape(ROWS, HEAD_DIM)
                q_off = q_ref[2 * sp:2 * sp + 2, GROUP:GROUP + 1, rows_at, :].astype(F32)
                q_pos = jnp.broadcast_to(q_off + ramp[None, None], (2, GROUP, HALF, HEAD_DIM)).reshape(ROWS, HEAD_DIM)
                count = (i + 1) * wide
                s = lax.dot_general(
                    q, keys[0:count, :], (((1,), (1,)), ((), ())), preferred_element_type=F32
                ) * SCALE
                pieces = [s[:, c * HEAD_DIM:(c + 1) * HEAD_DIM] for c in range(count // HEAD_DIM)]
                for n in range(shards):
                    c = i * shards + n
                    pieces[c] = jnp.where(tables[n][i:i + 1, :] <= q_pos, pieces[c], NEVER)
                top = functools.reduce(jnp.maximum, pieces)
                top = jnp.max(top, axis=1, keepdims=True)
                if first:
                    new_max = jnp.broadcast_to(jnp.maximum(top, LOWEST), (ROWS, HEAD_DIM))
                else:
                    old_max = old_refs[2 * half][b]
                    new_max = jnp.maximum(old_max, top)
                weights = jnp.concatenate([jnp.exp2(piece - new_max).astype(BF16) for piece in pieces], axis=1)
                sums = jnp.dot(weights, vals[0:count, :], preferred_element_type=F32)
                if not first:
                    rescale = jnp.exp2(old_max - new_max)
                    sums = sums + old_refs[2 * half + 1][b] * jnp.concatenate([rescale, rescale], axis=1)
                if last and half == 1:
                    lane = iota((ROWS, HEAD_DIM), 1)
                    new_refs[2][b, :, 0:HEAD_DIM] = sums[:, 0:HEAD_DIM]
                    new_refs[2][b, :, HEAD_DIM:] = jnp.where(lane < HEAD_DIM // 2, new_max, sums[:, HEAD_DIM:])
                else:
                    new_refs[2 * half][b] = new_max
                    new_refs[2 * half + 1][b] = sums


def attend(limit, qa, qb, parts, state, last=False):
    shards = len(parts)
    wide = shards * HEAD_DIM
    stats = jax.ShapeDtypeStruct((4, ROWS, HEAD_DIM), F32)
    sums = jax.ShapeDtypeStruct((4, ROWS, 2 * HEAD_DIM), F32)
    shapes = (stats, sums, sums) if last else (stats, sums, stats, sums)
    first = state is None
    held = [] if first else list(state)
    score_count = 4 * 2 * ROWS * 3 * wide
    base = 3 + shards
    return pl.pallas_call(
        functools.partial(attend_kernel, shards, first, last),
        out_shape=shapes,
        in_specs=[pl.BlockSpec(memory_space=pltpu.SMEM)] + [pl.BlockSpec(memory_space=VMEM)] * (2 + shards + len(held)),
        out_specs=(pl.BlockSpec(memory_space=VMEM),) * len(shapes),
        scratch_shapes=[VMEM((2 * wide, HEAD_DIM), BF16), VMEM((2 * wide, 2 * HEAD_DIM), BF16)],
        input_output_aliases={} if first else ({base: 0, base + 1: 1, base + 3: 2} if last else {base + n: n for n in range(4)}),
        compiler_params=pltpu.CompilerParams(vmem_limit_bytes=16 * 1024 * 1024),
        cost_estimate=pl.CostEstimate(
            flops=score_count * HEAD_DIM * 6, bytes_accessed=4_000_000, transcendentals=score_count
        ),
        name="attend_last" if last else "attend",
    )(limit, qa, qb, *parts, *held)


def hold_kernel(weight_ref, held_ref, arrived):
    copy = pltpu.make_async_copy(weight_ref, held_ref, arrived)
    copy.start()
    copy.wait()


def hold(weight):
    return pl.pallas_call(
        hold_kernel,
        out_shape=jax.ShapeDtypeStruct(weight.shape, weight.dtype),
        in_specs=[pl.BlockSpec(memory_space=pl.ANY)],
        out_specs=pl.BlockSpec(memory_space=VMEM),
        scratch_shapes=[pltpu.SemaphoreType.DMA],
        compiler_params=pltpu.CompilerParams(vmem_limit_bytes=10 * 1024 * 1024),
        cost_estimate=pl.CostEstimate(flops=2_000_000_000, bytes_accessed=8_000_000, transcendentals=0),
        name="hold",
    )(weight)


def merge_kernel(max_ref, sum_ref, got_ref, out_ref):
    for i in range(2):
        for sp in range(2):
            b = i * 2 + sp
            max_a = max_ref[b]
            max_b = jnp.broadcast_to(got_ref[b, :, HEAD_DIM:HEAD_DIM + 1], (ROWS, HEAD_DIM))
            total_b = jnp.broadcast_to(got_ref[b, :, 2 * HEAD_DIM - 1:], (ROWS, HEAD_DIM))
            top = jnp.maximum(max_a, max_b)
            part_a = jnp.exp2(max_a - top)
            part_b = jnp.exp2(max_b - top)
            total = sum_ref[b, :, HEAD_DIM:] * part_a + total_b * part_b
            value = sum_ref[b, :, 0:HEAD_DIM] * part_a + got_ref[b, :, 0:HEAD_DIM] * part_b
            value = (value / total).astype(BF16).reshape(2, GROUP, HALF, HEAD_DIM)
            out_ref[2 * sp:2 * sp + 2, :, HALF * i:HALF * (i + 1), :] = value


def merge(maxima, sums, got):
    return pl.pallas_call(
        merge_kernel,
        out_shape=jax.ShapeDtypeStruct((KV_HEADS, GROUP, TOK, HEAD_DIM), BF16),
        in_specs=[pl.BlockSpec(memory_space=VMEM)] * 3,
        out_specs=pl.BlockSpec(memory_space=VMEM),
        compiler_params=pltpu.CompilerParams(vmem_limit_bytes=12 * 1024 * 1024),
        cost_estimate=pl.CostEstimate(flops=4_000_000, bytes_accessed=3_000_000, transcendentals=300_000),
        name="merge",
    )(maxima, sums, got)


def project_kernel(member_ref, pos_ref, *refs):
    parts = refs[:KV_HEADS]
    weight_ref, residual_ref, out_ref, heads = refs[KV_HEADS:]
    member = member_ref[0]
    for d, part in enumerate(parts):
        heads[lax.rem(member + d, KV_HEADS)] = part[...]
    run = pos_ref[...] // RUN
    put = (jnp.broadcast_to(run, (TOK, TOK)) == iota((TOK, TOK), 1)).astype(F32).astype(BF16)
    rows = jnp.concatenate([heads[h, g] for h in range(KV_HEADS) for g in range(GROUP)], axis=1)
    rows = jnp.dot(put, rows, preferred_element_type=F32).astype(BF16)
    wide = 512
    for n in range(weight_ref.shape[1] // wide):
        cols = slice(n * wide, (n + 1) * wide)
        total = jnp.dot(rows, weight_ref[:, cols], preferred_element_type=F32)
        out_ref[:, cols] = (total + residual_ref[:, cols].astype(F32)).astype(BF16)


def project(member, positions, parts, out_weight, residual):
    return pl.pallas_call(
        project_kernel,
        out_shape=jax.ShapeDtypeStruct(residual.shape, BF16),
        in_specs=[pl.BlockSpec(memory_space=pltpu.SMEM)] + [pl.BlockSpec(memory_space=VMEM)] * (len(parts) + 3),
        out_specs=pl.BlockSpec(memory_space=VMEM),
        scratch_shapes=[VMEM((KV_HEADS, GROUP, TOK, HEAD_DIM), BF16)],
        compiler_params=pltpu.CompilerParams(vmem_limit_bytes=12 * 1024 * 1024),
        cost_estimate=pl.CostEstimate(flops=TOK * 2048 * 4096, bytes_accessed=9_000_000, transcendentals=0),
        name="project",
    )(member, positions.reshape(TOK, 1), *parts, out_weight, residual)


def on_device(seq_size, query_rows, key_rows, value_rows, positions, prompt_length, out_weight, residual):
    z_dev = seq_size // (X_DEV * CORES)

    def at(z, x, c):
        return ((z % z_dev) * X_DEV + x % X_DEV) * CORES + c % CORES

    spots = [(z, x, c) for z in range(z_dev) for x in range(X_DEV) for c in range(CORES)]

    def move(a, dz=0, dx=0, dc=0):
        return lax.ppermute(a, "seq", [(at(z, x, c), at(z + dz, x + dx, c + dc)) for z, x, c in spots])

    def turn(a, d):
        return lax.ppermute(
            a, "seq", [(at(z, x, c), at(z // BLOCK * BLOCK + (z + d) % BLOCK, x, c)) for z, x, c in spots]
        )

    member = lax.rem(lax.axis_index("seq") // (X_DEV * CORES), BLOCK)

    def exchange(a):
        pick = [lax.dynamic_index_in_dim(a, lax.rem(member + d, BLOCK), 0, keepdims=False) for d in range(BLOCK)]
        return [pick[0]] + [turn(pick[d], d) for d in range(1, BLOCK)]

    qs, kvs = prep(positions, query_rows, key_rows, value_rows)
    own = jnp.stack(exchange(kvs))

    def spread(a):
        return [a, move(a, dx=1), move(a, dx=-1), move(a, dx=2)]

    ahead = move(own, dz=BLOCK)
    behind = move(own, dz=-BLOCK)
    across = move(own, dz=2 * BLOCK)
    group = spread(own)
    qs, own = lax.optimization_barrier((qs, own))
    qa = jnp.stack(exchange(qs))
    qb = move(qa, dc=1)
    state = attend(prompt_length, qa, qb, group, None)
    state, ahead, behind = lax.optimization_barrier((state, ahead, behind))
    next_group, group = spread(ahead), spread(behind)
    state = attend(prompt_length, qa, qb, next_group, state)
    state, across = lax.optimization_barrier((state, across))
    last_group = spread(across)
    state = attend(prompt_length, qa, qb, group, state)
    state = attend(prompt_length, qa, qb, last_group, state, last=True)
    got = move(state[2], dc=1)
    done = merge(state[0], state[1], got)
    parts = [done[0]] + [turn(done[d], -d) for d in range(1, BLOCK)]
    weight, done = lax.optimization_barrier((out_weight, done))
    weight = hold(weight)
    return project(member.reshape(1), positions, parts, weight, residual)


def solution(mesh):
    def step(*args):
        return on_device(mesh.shape["seq"], *args)

    return jax.shard_map(
        step,
        mesh=mesh,
        in_specs=(
            P(("groups", "seq"), None),
            P(("groups", "seq"), None),
            P(("groups", "seq"), None),
            P(("groups", "seq")),
            P("groups"),
            P(),
            P(("groups", "seq"), None),
        ),
        out_specs=P(("groups", "seq"), None),
        check_vma=False,
    )
```

```python
import functools
import math
import jax
import jax.numpy as jnp
from jax import lax
from jax.experimental import pallas as pl
from jax.experimental.pallas import tpu as pltpu
from jax.sharding import PartitionSpec as P

HEADS = 16
KV_HEADS = 4
HEAD_DIM = 128
GROUP = HEADS // KV_HEADS
TOK = 64
RUN = 128
X_DEV = 4
CORES = 2
BLOCK = KV_HEADS
HALF = 32
KV_ROWS = 2 * TOK + 8
ALL_ROWS = (2 + GROUP) * TOK + 8
ROWS = 256
SCALE = HEAD_DIM ** -0.5 * math.log2(math.e)
NEVER = -1e30
LOWEST = -1e20
VMEM = pltpu.VMEM
F32 = jnp.float32
BF16 = jnp.bfloat16


def iota(shape, dim):
    return lax.broadcasted_iota(jnp.int32, shape, dim)


def prep_kernel(pos_hbm, q_hbm, k_hbm, v_hbm, out_ref, pos_ref, q_ref, k_ref, v_ref, arrived):
    copies = [
        pltpu.make_async_copy(source, target, arrived.at[n])
        for n, (source, target) in enumerate(
            ((pos_hbm, pos_ref), (k_hbm, k_ref), (v_hbm, v_ref), (q_hbm, q_ref))
        )
    ]
    for copy in copies:
        copy.start()
    copies[0].wait()
    pos = pos_ref[...]
    run = pos // RUN
    off = (pos - run * RUN).astype(F32)
    pick = (iota((TOK, TOK), 0) == jnp.broadcast_to(run, (TOK, TOK))).astype(F32)
    pick16 = pick.astype(BF16)
    off_col = jnp.dot(
        (pick * jnp.broadcast_to(off, (TOK, TOK))).astype(BF16),
        jnp.ones((TOK, HEAD_DIM), BF16),
        preferred_element_type=F32,
    )
    row = iota((TOK, HEAD_DIM), 0)
    lane = iota((TOK, HEAD_DIM), 1)
    lines = [
        jnp.sum(jnp.where(row == HALF * j + lane % HALF, off_col, 0.0), axis=0, keepdims=True)
        for j in range(TOK // HALF)
    ]
    table = jnp.concatenate(lines + [jnp.zeros((8 - len(lines), HEAD_DIM), F32)], axis=0).astype(BF16)
    copies[1].wait()
    sorted_k = jnp.dot(pick16, k_ref[...], preferred_element_type=F32).astype(BF16)
    copies[2].wait()
    sorted_v = jnp.dot(pick16, v_ref[...], preferred_element_type=F32).astype(BF16)
    copies[3].wait()
    sorted_q = jnp.dot(pick16, q_ref[...], preferred_element_type=F32).astype(BF16)
    for h in range(KV_HEADS):
        cols = slice(h * HEAD_DIM, (h + 1) * HEAD_DIM)
        out_ref[h, 0:TOK, :] = sorted_k[:, cols]
        out_ref[h, TOK:2 * TOK, :] = sorted_v[:, cols]
        for g in range(GROUP):
            at = (h * GROUP + g) * HEAD_DIM
            out_ref[h, (2 + g) * TOK:(3 + g) * TOK, :] = sorted_q[:, at:at + HEAD_DIM]
        out_ref[h, (2 + GROUP) * TOK:ALL_ROWS, :] = table


def prep(positions, query_rows, key_rows, value_rows):
    return pl.pallas_call(
        prep_kernel,
        out_shape=jax.ShapeDtypeStruct((KV_HEADS, ALL_ROWS, HEAD_DIM), BF16),
        in_specs=[pl.BlockSpec(memory_space=pltpu.HBM)] * 4,
        out_specs=pl.BlockSpec(memory_space=VMEM),
        scratch_shapes=[
            VMEM((1, TOK), jnp.int32),
            VMEM(query_rows.shape, BF16),
            VMEM(key_rows.shape, BF16),
            VMEM(value_rows.shape, BF16),
            pltpu.SemaphoreType.DMA((4,)),
        ],
        compiler_params=pltpu.CompilerParams(vmem_limit_bytes=60 * 1024 * 1024),
        cost_estimate=pl.CostEstimate(flops=TOK * TOK * 3072 * 2, bytes_accessed=800_000, transcendentals=0),
        name="prep",
    )(positions.reshape(1, TOK), query_rows, key_rows, value_rows)


def attend_kernel(parts, first, last, *refs):
    limit_ref, qa_ref, qb_ref = refs[:3]
    kv_refs = refs[3:3 + parts]
    refs = refs[3 + parts:]
    if first:
        old_refs = None
    else:
        old_refs, refs = refs[:4], refs[4:]
    new_refs, (keys, vals) = refs[:-2], refs[-2:]
    limit = limit_ref[0]
    sources = KV_HEADS
    units = [(kv, at) for kv in kv_refs for at in range(0, kv.shape[0], sources)]
    shards = len(units)
    wide = shards * HEAD_DIM
    for j in range(2):
        for n, (kv, base) in enumerate(units):
            for s in range(sources):
                at = j * wide + (n * sources + s) * HALF
                keys[at:at + HALF, :] = kv[base + s, HALF * j:HALF * (j + 1), :]
                vals[at:at + HALF, 0:HEAD_DIM] = kv[base + s, TOK + HALF * j:TOK + HALF * (j + 1), :]
    vals[:, HEAD_DIM:] = jnp.ones((2 * wide, HEAD_DIM), BF16)
    lane8 = iota((8, HEAD_DIM), 1)
    tables = []
    for kv, base in units:
        table = kv[base, 2 * TOK:KV_ROWS, :].astype(F32)
        for s in range(1, sources):
            table = jnp.where(lane8 // HALF == s, kv[base + s, 2 * TOK:KV_ROWS, :].astype(F32), table)
        table = table + (lane8 % HALF * RUN).astype(F32)
        chunk = (iota((8, HEAD_DIM), 0) * (HALF * RUN)).astype(F32)
        tables.append(jnp.where(table + chunk >= limit.astype(F32), 1e9, table))
    ramp = (iota((HALF, HEAD_DIM), 0) * RUN).astype(F32)
    diagonal = iota((HALF, HEAD_DIM), 0) == iota((HALF, HEAD_DIM), 1)
    spread = [
        jnp.where(diagonal, q_ref[src, ALL_ROWS - 8 + i:ALL_ROWS - 7 + i, :].astype(F32), 0.0).astype(BF16)
        for q_ref in (qa_ref, qb_ref)
        for i in range(2)
        for src in range(sources)
    ]
    offsets = jnp.dot(
        jnp.concatenate(spread, axis=0), jnp.ones((HEAD_DIM, HEAD_DIM), BF16), preferred_element_type=F32
    )
    for half, q_ref in enumerate((qa_ref, qb_ref)):
        for i in range(2):
            for sp in range(2):
                b = i * 2 + sp
                q_rows = []
                q_poss = []
                for src in (2 * sp, 2 * sp + 1):
                    for g in range(GROUP):
                        at = (2 + g) * TOK + HALF * i
                        q_rows.append(q_ref[src, at:at + HALF, :])
                    at = ((half * 2 + i) * sources + src) * HALF
                    q_poss += [offsets[at:at + HALF, :] + ramp] * GROUP
                q = jnp.concatenate(q_rows, axis=0)
                q_pos = jnp.concatenate(q_poss, axis=0)
                count = (i + 1) * wide
                s = lax.dot_general(
                    q, keys[0:count, :], (((1,), (1,)), ((), ())), preferred_element_type=F32
                ) * SCALE
                pieces = [s[:, c * HEAD_DIM:(c + 1) * HEAD_DIM] for c in range(count // HEAD_DIM)]
                for n in range(shards):
                    c = i * shards + n
                    pieces[c] = jnp.where(tables[n][i:i + 1, :] <= q_pos, pieces[c], NEVER)
                top = functools.reduce(jnp.maximum, pieces)
                top = jnp.max(top, axis=1, keepdims=True)
                if first:
                    new_max = jnp.broadcast_to(jnp.maximum(top, LOWEST), (ROWS, HEAD_DIM))
                else:
                    old_max = old_refs[2 * half][b]
                    new_max = jnp.maximum(old_max, top)
                weights = jnp.concatenate([jnp.exp2(piece - new_max).astype(BF16) for piece in pieces], axis=1)
                sums = jnp.dot(weights, vals[0:count, :], preferred_element_type=F32)
                if not first:
                    rescale = jnp.exp2(old_max - new_max)
                    sums = sums + old_refs[2 * half + 1][b] * jnp.concatenate([rescale, rescale], axis=1)
                if last and half == 1:
                    lane = iota((ROWS, HEAD_DIM), 1)
                    new_refs[2][b, :, 0:HEAD_DIM] = sums[:, 0:HEAD_DIM]
                    new_refs[2][b, :, HEAD_DIM:] = jnp.where(lane < HEAD_DIM // 2, new_max, sums[:, HEAD_DIM:])
                else:
                    new_refs[2 * half][b] = new_max
                    new_refs[2 * half + 1][b] = sums


def attend(limit, qa, qb, parts, state, last=False):
    shards = sum(part.shape[0] for part in parts) // KV_HEADS
    wide = shards * HEAD_DIM
    stats = jax.ShapeDtypeStruct((4, ROWS, HEAD_DIM), F32)
    sums = jax.ShapeDtypeStruct((4, ROWS, 2 * HEAD_DIM), F32)
    shapes = (stats, sums, sums) if last else (stats, sums, stats, sums)
    first = state is None
    held = [] if first else list(state)
    score_count = 4 * 2 * ROWS * 3 * wide
    base = 3 + len(parts)
    return pl.pallas_call(
        functools.partial(attend_kernel, len(parts), first, last),
        out_shape=shapes,
        in_specs=[pl.BlockSpec(memory_space=pltpu.SMEM)] + [pl.BlockSpec(memory_space=VMEM)] * (2 + len(parts) + len(held)),
        out_specs=(pl.BlockSpec(memory_space=VMEM),) * len(shapes),
        scratch_shapes=[VMEM((2 * wide, HEAD_DIM), BF16), VMEM((2 * wide, 2 * HEAD_DIM), BF16)],
        input_output_aliases={} if first else ({base: 0, base + 1: 1} if last else {base + n: n for n in range(4)}),
        compiler_params=pltpu.CompilerParams(vmem_limit_bytes=12 * 1024 * 1024),
        cost_estimate=pl.CostEstimate(
            flops=score_count * HEAD_DIM * 6, bytes_accessed=4_000_000, transcendentals=score_count
        ),
        name="attend_last" if last else "attend",
    )(limit, qa, qb, *parts, *held)


def hold_kernel(weight_ref, held_ref, arrived):
    copy = pltpu.make_async_copy(weight_ref, held_ref, arrived)
    copy.start()
    copy.wait()


def hold(weight):
    return pl.pallas_call(
        hold_kernel,
        out_shape=jax.ShapeDtypeStruct(weight.shape, weight.dtype),
        in_specs=[pl.BlockSpec(memory_space=pl.ANY)],
        out_specs=pl.BlockSpec(memory_space=VMEM),
        scratch_shapes=[pltpu.SemaphoreType.DMA],
        compiler_params=pltpu.CompilerParams(vmem_limit_bytes=10 * 1024 * 1024),
        cost_estimate=pl.CostEstimate(flops=2_000_000_000, bytes_accessed=8_000_000, transcendentals=0),
        name="hold",
    )(weight)


def merge_kernel(max_ref, sum_ref, got_ref, out_ref):
    for i in range(2):
        for sp in range(2):
            b = i * 2 + sp
            max_a = max_ref[b]
            max_b = jnp.broadcast_to(got_ref[b, :, HEAD_DIM:HEAD_DIM + 1], (ROWS, HEAD_DIM))
            total_b = jnp.broadcast_to(got_ref[b, :, 2 * HEAD_DIM - 1:], (ROWS, HEAD_DIM))
            top = jnp.maximum(max_a, max_b)
            part_a = jnp.exp2(max_a - top)
            part_b = jnp.exp2(max_b - top)
            total = sum_ref[b, :, HEAD_DIM:] * part_a + total_b * part_b
            value = sum_ref[b, :, 0:HEAD_DIM] * part_a + got_ref[b, :, 0:HEAD_DIM] * part_b
            value = (value / total).astype(BF16).reshape(2, GROUP, HALF, HEAD_DIM)
            out_ref[2 * sp:2 * sp + 2, :, HALF * i:HALF * (i + 1), :] = value


def merge(maxima, sums, got):
    return pl.pallas_call(
        merge_kernel,
        out_shape=jax.ShapeDtypeStruct((KV_HEADS, GROUP, TOK, HEAD_DIM), BF16),
        in_specs=[pl.BlockSpec(memory_space=VMEM)] * 3,
        out_specs=pl.BlockSpec(memory_space=VMEM),
        compiler_params=pltpu.CompilerParams(vmem_limit_bytes=12 * 1024 * 1024),
        cost_estimate=pl.CostEstimate(flops=4_000_000, bytes_accessed=3_000_000, transcendentals=300_000),
        name="merge",
    )(maxima, sums, got)


def project_kernel(member_ref, pos_ref, *refs):
    parts = refs[:KV_HEADS]
    weight_ref, residual_ref, out_ref, heads = refs[KV_HEADS:]
    member = member_ref[0]
    for d, part in enumerate(parts):
        heads[lax.rem(member + d, KV_HEADS)] = part[...]
    run = pos_ref[...] // RUN
    put = (jnp.broadcast_to(run, (TOK, TOK)) == iota((TOK, TOK), 1)).astype(F32).astype(BF16)
    rows = jnp.concatenate([heads[h, g] for h in range(KV_HEADS) for g in range(GROUP)], axis=1)
    rows = jnp.dot(put, rows, preferred_element_type=F32).astype(BF16)
    wide = 512
    for n in range(weight_ref.shape[1] // wide):
        cols = slice(n * wide, (n + 1) * wide)
        total = jnp.dot(rows, weight_ref[:, cols], preferred_element_type=F32)
        out_ref[:, cols] = (total + residual_ref[:, cols].astype(F32)).astype(BF16)


def project(member, positions, parts, out_weight, residual):
    return pl.pallas_call(
        project_kernel,
        out_shape=jax.ShapeDtypeStruct(residual.shape, BF16),
        in_specs=[pl.BlockSpec(memory_space=pltpu.SMEM)] + [pl.BlockSpec(memory_space=VMEM)] * (len(parts) + 3),
        out_specs=pl.BlockSpec(memory_space=VMEM),
        scratch_shapes=[VMEM((KV_HEADS, GROUP, TOK, HEAD_DIM), BF16)],
        compiler_params=pltpu.CompilerParams(vmem_limit_bytes=12 * 1024 * 1024),
        cost_estimate=pl.CostEstimate(flops=TOK * 2048 * 4096, bytes_accessed=9_000_000, transcendentals=0),
        name="project",
    )(member, positions.reshape(TOK, 1), *parts, out_weight, residual)


def on_device(seq_size, query_rows, key_rows, value_rows, positions, prompt_length, out_weight, residual):
    z_dev = seq_size // (X_DEV * CORES)

    def at(z, x, c):
        return ((z % z_dev) * X_DEV + x % X_DEV) * CORES + c % CORES

    spots = [(z, x, c) for z in range(z_dev) for x in range(X_DEV) for c in range(CORES)]

    def move(a, dz=0, dx=0, dc=0):
        return lax.ppermute(a, "seq", [(at(z, x, c), at(z + dz, x + dx, c + dc)) for z, x, c in spots])

    def far(a):
        return lax.ppermute(
            a, "seq", [(at(z, x, c), at(z + (BLOCK if c == 0 else -BLOCK), x, c)) for z, x, c in spots]
        )

    def turn(a, d):
        return lax.ppermute(
            a, "seq", [(at(z, x, c), at(z // BLOCK * BLOCK + (z + d) % BLOCK, x, c)) for z, x, c in spots]
        )

    def spread(a):
        return [move(a, dx=2), move(a, dx=1), move(a, dx=-1)]

    member = lax.rem(lax.axis_index("seq") // (X_DEV * CORES), BLOCK)
    message = prep(positions, query_rows, key_rows, value_rows)
    pick = [lax.dynamic_index_in_dim(message, lax.rem(member + d, BLOCK), 0, keepdims=False) for d in range(BLOCK)]
    own = jnp.stack([pick[0]] + [turn(pick[d], d) for d in range(1, BLOCK)])
    twin = move(own, dc=1)

    def kv_of(a):
        return jnp.concatenate([a[:, 0:2 * TOK], a[:, ALL_ROWS - 8:]], axis=1)

    mine = kv_of(own)
    one = far(mine)
    other = far(kv_of(twin))
    group = [mine] + spread(mine)
    two = far(one)
    state = attend(prompt_length, own, twin, group, None)
    state, other = lax.optimization_barrier((state, other))
    one = jnp.concatenate([one, other], axis=0)
    group = [one] + spread(one)
    state = attend(prompt_length, own, twin, group[:2], state)
    state, two = lax.optimization_barrier((state, two))
    last_group = spread(two)
    state = attend(prompt_length, own, twin, group[2:] + [two], state)
    state = attend(prompt_length, own, twin, last_group, state, last=True)
    got = move(state[2], dc=1)
    done = merge(state[0], state[1], got)
    parts = [done[0]] + [turn(done[d], -d) for d in range(1, BLOCK)]
    weight, done = lax.optimization_barrier((out_weight, done))
    weight = hold(weight)
    return project(member.reshape(1), positions, parts, weight, residual)


def solution(mesh):
    def step(*args):
        return on_device(mesh.shape["seq"], *args)

    return jax.shard_map(
        step,
        mesh=mesh,
        in_specs=(
            P(("groups", "seq"), None),
            P(("groups", "seq"), None),
            P(("groups", "seq"), None),
            P(("groups", "seq")),
            P("groups"),
            P(),
            P(("groups", "seq"), None),
        ),
        out_specs=P(("groups", "seq"), None),
        check_vma=False,
    )
```

```python
import functools
import math
import jax
import jax.numpy as jnp
from jax import lax
from jax.experimental import pallas as pl
from jax.experimental.pallas import tpu as pltpu
from jax.sharding import PartitionSpec as P

HEADS = 16
KV_HEADS = 4
HEAD_DIM = 128
GROUP = HEADS // KV_HEADS
TOK = 64
RUN = 128
X_DEV = 4
CORES = 2
BLOCK = KV_HEADS
HALF = 32
KV_ROWS = 2 * TOK + 8
ALL_ROWS = (2 + GROUP) * TOK + 8
TOGETHER = 4
ROWS = TOGETHER * GROUP * HALF
PAIRS = KV_HEADS // TOGETHER
SCALE = HEAD_DIM ** -0.5 * math.log2(math.e)
PART = 32
NEVER = -1e30
LOWEST = -1e20
VMEM = pltpu.VMEM
F32 = jnp.float32
BF16 = jnp.bfloat16


def iota(shape, dim):
    return lax.broadcasted_iota(jnp.int32, shape, dim)


def prep_kernel(pos_hbm, q_hbm, k_hbm, v_hbm, out_ref, pos_ref, q_ref, k_ref, v_ref, arrived):
    copies = [
        pltpu.make_async_copy(source, target, arrived.at[n])
        for n, (source, target) in enumerate(
            ((pos_hbm, pos_ref), (k_hbm, k_ref), (v_hbm, v_ref), (q_hbm, q_ref))
        )
    ]
    for copy in copies:
        copy.start()
    copies[0].wait()
    pos = pos_ref[...]
    run = pos // RUN
    off = (pos - run * RUN).astype(F32)
    pick = (iota((TOK, TOK), 0) == jnp.broadcast_to(run, (TOK, TOK))).astype(F32)
    pick16 = pick.astype(BF16)
    off_col = jnp.dot(
        (pick * jnp.broadcast_to(off, (TOK, TOK))).astype(BF16),
        jnp.ones((TOK, HEAD_DIM), BF16),
        preferred_element_type=F32,
    )
    row = iota((TOK, HEAD_DIM), 0)
    lane = iota((TOK, HEAD_DIM), 1)
    lines = [
        jnp.sum(jnp.where(row == HALF * j + lane % HALF, off_col, 0.0), axis=0, keepdims=True)
        for j in range(TOK // HALF)
    ]
    table = jnp.concatenate(lines + [jnp.zeros((8 - len(lines), HEAD_DIM), F32)], axis=0).astype(BF16)
    copies[1].wait()
    sorted_k = jnp.dot(pick16, k_ref[...], preferred_element_type=F32).astype(BF16)
    copies[2].wait()
    sorted_v = jnp.dot(pick16, v_ref[...], preferred_element_type=F32).astype(BF16)
    copies[3].wait()
    sorted_q = jnp.dot(pick16, q_ref[...], preferred_element_type=F32).astype(BF16)
    for h in range(KV_HEADS):
        cols = slice(h * HEAD_DIM, (h + 1) * HEAD_DIM)
        out_ref[h, 0:TOK, :] = sorted_k[:, cols]
        out_ref[h, TOK:2 * TOK, :] = sorted_v[:, cols]
        for g in range(GROUP):
            at = (h * GROUP + g) * HEAD_DIM
            out_ref[h, (2 + g) * TOK:(3 + g) * TOK, :] = sorted_q[:, at:at + HEAD_DIM]
        out_ref[h, (2 + GROUP) * TOK:ALL_ROWS, :] = table


def in_hbm(a):
    return pltpu.with_memory_space_constraint(a, pltpu.HBM)


def prep(positions, query_rows, key_rows, value_rows):
    return pl.pallas_call(
        prep_kernel,
        out_shape=VMEM((KV_HEADS, ALL_ROWS, HEAD_DIM), BF16),
        in_specs=[pl.BlockSpec(memory_space=pltpu.HBM)] * 4,
        out_specs=pl.BlockSpec(memory_space=VMEM),
        scratch_shapes=[
            VMEM((1, TOK), jnp.int32),
            VMEM(query_rows.shape, BF16),
            VMEM(key_rows.shape, BF16),
            VMEM(value_rows.shape, BF16),
            pltpu.SemaphoreType.DMA((4,)),
        ],
        compiler_params=pltpu.CompilerParams(vmem_limit_bytes=8 * 1024 * 1024),
        cost_estimate=pl.CostEstimate(flops=TOK * TOK * 3072 * 2, bytes_accessed=800_000, transcendentals=0),
        name="prep",
    )(*(in_hbm(a) for a in (positions.reshape(1, TOK), query_rows, key_rows, value_rows)))


def attend_kernel(parts, first, last, *refs):
    limit_ref, qa_ref, qb_ref = refs[:3]
    kv_refs = refs[3:3 + parts]
    refs = refs[3 + parts:]
    if first:
        old_refs = None
    else:
        old_refs, refs = refs[:4], refs[4:]
    new_refs, (keys, vals) = refs[:-2], refs[-2:]
    limit = limit_ref[0]
    sources = KV_HEADS
    units = [(kv, at) for kv in kv_refs for at in range(0, kv.shape[0], sources)]
    shards = len(units)
    wide = shards * HEAD_DIM
    for j in range(2):
        for n, (kv, base) in enumerate(units):
            for s in range(sources):
                at = j * wide + (n * sources + s) * HALF
                keys[at:at + HALF, :] = kv[base + s, HALF * j:HALF * (j + 1), :]
                vals[at:at + HALF, 0:HEAD_DIM] = kv[base + s, TOK + HALF * j:TOK + HALF * (j + 1), :]
    vals[:, HEAD_DIM:] = jnp.ones((2 * wide, HEAD_DIM), BF16)
    lane8 = iota((8, HEAD_DIM), 1)
    tables = []
    for kv, base in units:
        table = kv[base, 2 * TOK:KV_ROWS, :].astype(F32)
        for s in range(1, sources):
            table = jnp.where(lane8 // HALF == s, kv[base + s, 2 * TOK:KV_ROWS, :].astype(F32), table)
        table = table + (lane8 % HALF * RUN).astype(F32)
        chunk = (iota((8, HEAD_DIM), 0) * (HALF * RUN)).astype(F32)
        tables.append(jnp.where(table + chunk >= limit.astype(F32), 1e9, table))
    ramp = (iota((HALF, HEAD_DIM), 0) * RUN).astype(F32)
    diagonal = iota((HALF, HEAD_DIM), 0) == iota((HALF, HEAD_DIM), 1)
    spread = [
        jnp.where(diagonal, q_ref[src, ALL_ROWS - 8 + i:ALL_ROWS - 7 + i, :].astype(F32), 0.0).astype(BF16)
        for q_ref in (qa_ref, qb_ref)
        for i in range(2)
        for src in range(sources)
    ]
    offsets = jnp.dot(
        jnp.concatenate(spread, axis=0), jnp.ones((HEAD_DIM, HEAD_DIM), BF16), preferred_element_type=F32
    )
    for half, q_ref in enumerate((qa_ref, qb_ref)):
        for i in range(2):
            for sp in range(PAIRS):
                b = i * PAIRS + sp
                q_rows = []
                q_poss = []
                for src in range(TOGETHER * sp, TOGETHER * (sp + 1)):
                    for g in range(GROUP):
                        at = (2 + g) * TOK + HALF * i
                        q_rows.append(q_ref[src, at:at + HALF, :])
                    at = ((half * 2 + i) * sources + src) * HALF
                    q_poss += [offsets[at:at + HALF, :] + ramp] * GROUP
                q = jnp.concatenate(q_rows, axis=0)
                q_pos = jnp.concatenate(q_poss, axis=0)
                count = (i + 1) * wide
                s = lax.dot_general(
                    q, keys[0:count, :], (((1,), (1,)), ((), ())), preferred_element_type=F32
                ) * SCALE
                pieces = [s[:, c * HEAD_DIM:(c + 1) * HEAD_DIM] for c in range(count // HEAD_DIM)]
                for n in range(shards):
                    c = i * shards + n
                    pieces[c] = jnp.where(tables[n][i:i + 1, :] <= q_pos, pieces[c], NEVER)
                top = functools.reduce(jnp.maximum, pieces)
                top = jnp.max(top, axis=1, keepdims=True)
                if first:
                    new_max = jnp.broadcast_to(jnp.maximum(top, LOWEST), (ROWS, HEAD_DIM))
                else:
                    old_max = old_refs[2 * half][b]
                    new_max = jnp.maximum(old_max, top)
                weights = jnp.concatenate([jnp.exp2(piece - new_max).astype(BF16) for piece in pieces], axis=1)
                sums = jnp.dot(weights, vals[0:count, :], preferred_element_type=F32)
                if not first:
                    rescale = jnp.exp2(old_max - new_max)
                    sums = sums + old_refs[2 * half + 1][b] * jnp.concatenate([rescale, rescale], axis=1)
                if last and half == 1:
                    lane = iota((ROWS, HEAD_DIM), 1)
                    total = jnp.maximum(sums[:, HEAD_DIM:], 1e-30)
                    level = new_max + jnp.log2(total)
                    high = level.astype(BF16).astype(F32)
                    middle = (level - high).astype(BF16).astype(F32)
                    parts3 = jnp.where(lane < PART, high, jnp.where(lane < 2 * PART, middle, level - high - middle))
                    new_refs[2][b, :, 0:HEAD_DIM] = (sums[:, 0:HEAD_DIM] / total).astype(BF16)
                    new_refs[2][b, :, HEAD_DIM:] = parts3.astype(BF16)
                else:
                    new_refs[2 * half][b] = new_max
                    new_refs[2 * half + 1][b] = sums


def attend(limit, qa, qb, parts, state, last=False):
    shards = sum(part.shape[0] for part in parts) // KV_HEADS
    wide = shards * HEAD_DIM
    stats = jax.ShapeDtypeStruct((2 * PAIRS, ROWS, HEAD_DIM), F32)
    sums = jax.ShapeDtypeStruct((2 * PAIRS, ROWS, 2 * HEAD_DIM), F32)
    shapes = (stats, sums, VMEM(sums.shape, BF16)) if last else (stats, sums, stats, sums)
    first = state is None
    held = [] if first else list(state)
    score_count = 4 * 2 * 256 * 3 * wide
    base = 3 + len(parts)
    return pl.pallas_call(
        functools.partial(attend_kernel, len(parts), first, last),
        out_shape=shapes,
        in_specs=[pl.BlockSpec(memory_space=pltpu.SMEM)] + [pl.BlockSpec(memory_space=VMEM)] * (2 + len(parts) + len(held)),
        out_specs=(pl.BlockSpec(memory_space=VMEM),) * len(shapes),
        scratch_shapes=[VMEM((2 * wide, HEAD_DIM), BF16), VMEM((2 * wide, 2 * HEAD_DIM), BF16)],
        input_output_aliases={} if first else ({base: 0, base + 1: 1} if last else {base + n: n for n in range(4)}),
        compiler_params=pltpu.CompilerParams(vmem_limit_bytes=12 * 1024 * 1024),
        cost_estimate=pl.CostEstimate(
            flops=score_count * HEAD_DIM * 6, bytes_accessed=4_000_000, transcendentals=score_count
        ),
        name="attend_last" if last else "attend",
    )(limit, qa, qb, *parts, *held)


def hold_kernel(weight_ref, held_ref, arrived):
    copy = pltpu.make_async_copy(weight_ref, held_ref, arrived)
    copy.start()
    copy.wait()


def hold(weight):
    return pl.pallas_call(
        hold_kernel,
        out_shape=VMEM(weight.shape, weight.dtype),
        in_specs=[pl.BlockSpec(memory_space=pltpu.HBM)],
        out_specs=pl.BlockSpec(memory_space=VMEM),
        scratch_shapes=[pltpu.SemaphoreType.DMA],
        compiler_params=pltpu.CompilerParams(vmem_limit_bytes=10 * 1024 * 1024),
        cost_estimate=pl.CostEstimate(flops=2_000_000_000, bytes_accessed=8_000_000, transcendentals=0),
        name="hold",
    )(in_hbm(weight))


def merge_kernel(max_ref, sum_ref, got_ref, out_ref):
    for i in range(2):
        for sp in range(PAIRS):
            b = i * PAIRS + sp
            max_a = max_ref[b]
            level = got_ref[b, :, HEAD_DIM:].astype(F32)
            level = level[:, 0:1] + level[:, PART:PART + 1] + level[:, 2 * PART:2 * PART + 1]
            max_b = jnp.broadcast_to(level, (ROWS, HEAD_DIM))
            top = jnp.maximum(max_a, max_b)
            part_a = jnp.exp2(max_a - top)
            part_b = jnp.exp2(max_b - top)
            total = sum_ref[b, :, HEAD_DIM:] * part_a + part_b
            value = sum_ref[b, :, 0:HEAD_DIM] * part_a + got_ref[b, :, 0:HEAD_DIM].astype(F32) * part_b
            value = (value / total).astype(BF16).reshape(TOGETHER, GROUP, HALF, HEAD_DIM)
            out_ref[TOGETHER * sp:TOGETHER * (sp + 1), :, HALF * i:HALF * (i + 1), :] = value


def merge(maxima, sums, got):
    return pl.pallas_call(
        merge_kernel,
        out_shape=jax.ShapeDtypeStruct((KV_HEADS, GROUP, TOK, HEAD_DIM), BF16),
        in_specs=[pl.BlockSpec(memory_space=VMEM)] * 3,
        out_specs=pl.BlockSpec(memory_space=VMEM),
        compiler_params=pltpu.CompilerParams(vmem_limit_bytes=12 * 1024 * 1024),
        cost_estimate=pl.CostEstimate(flops=4_000_000, bytes_accessed=3_000_000, transcendentals=300_000),
        name="merge",
    )(maxima, sums, got)


def project_kernel(member_ref, pos_ref, *refs):
    parts = refs[:KV_HEADS]
    weight_ref, residual_ref, out_ref, heads = refs[KV_HEADS:]
    member = member_ref[0]
    for d, part in enumerate(parts):
        heads[lax.rem(member + d, KV_HEADS)] = part[...]
    run = pos_ref[...] // RUN
    put = (jnp.broadcast_to(run, (TOK, TOK)) == iota((TOK, TOK), 1)).astype(F32).astype(BF16)
    rows = jnp.concatenate([heads[h, g] for h in range(KV_HEADS) for g in range(GROUP)], axis=1)
    rows = jnp.dot(put, rows, preferred_element_type=F32).astype(BF16)
    wide = 512
    for n in range(weight_ref.shape[1] // wide):
        cols = slice(n * wide, (n + 1) * wide)
        total = jnp.dot(rows, weight_ref[:, cols], preferred_element_type=F32)
        out_ref[:, cols] = (total + residual_ref[:, cols].astype(F32)).astype(BF16)


def project(member, positions, parts, out_weight, residual):
    return pl.pallas_call(
        project_kernel,
        out_shape=jax.ShapeDtypeStruct(residual.shape, BF16),
        in_specs=[pl.BlockSpec(memory_space=pltpu.SMEM)] + [pl.BlockSpec(memory_space=VMEM)] * (len(parts) + 3),
        out_specs=pl.BlockSpec(memory_space=VMEM),
        scratch_shapes=[VMEM((KV_HEADS, GROUP, TOK, HEAD_DIM), BF16)],
        compiler_params=pltpu.CompilerParams(vmem_limit_bytes=12 * 1024 * 1024),
        cost_estimate=pl.CostEstimate(flops=TOK * 2048 * 4096, bytes_accessed=9_000_000, transcendentals=0),
        name="project",
    )(member, positions.reshape(TOK, 1), *parts, out_weight, residual)


def on_device(seq_size, query_rows, key_rows, value_rows, positions, prompt_length, out_weight, residual):
    z_dev = seq_size // (X_DEV * CORES)

    def at(z, x, c):
        return ((z % z_dev) * X_DEV + x % X_DEV) * CORES + c % CORES

    spots = [(z, x, c) for z in range(z_dev) for x in range(X_DEV) for c in range(CORES)]

    def move(a, dz=0, dx=0, dc=0):
        return lax.ppermute(a, "seq", [(at(z, x, c), at(z + dz, x + dx, c + dc)) for z, x, c in spots])

    def far(a):
        return lax.ppermute(
            a, "seq", [(at(z, x, c), at(z + (BLOCK if c == 0 else -BLOCK), x, c)) for z, x, c in spots]
        )

    def turn(a, d):
        return lax.ppermute(
            a, "seq", [(at(z, x, c), at(z // BLOCK * BLOCK + (z + d) % BLOCK, x, c)) for z, x, c in spots]
        )

    def spread(a):
        return [move(a, dx=1), move(a, dx=-1), move(a, dx=2)]

    member = lax.rem(lax.axis_index("seq") // (X_DEV * CORES), BLOCK)
    message = prep(positions, query_rows, key_rows, value_rows)
    pick = [lax.dynamic_index_in_dim(message, lax.rem(member + d, BLOCK), 0, keepdims=False) for d in range(BLOCK)]
    own = jnp.stack([pick[0]] + [turn(pick[d], d) for d in range(1, BLOCK)])
    twin = move(own, dc=1)

    def kv_of(a):
        return jnp.concatenate([a[:, 0:2 * TOK], a[:, ALL_ROWS - 8:]], axis=1)

    mine = kv_of(own)
    one = far(mine)
    other = far(kv_of(twin))
    own_group = [mine] + spread(mine)
    two = far(one)
    one_group = [one] + spread(one)
    other_group = [other] + spread(other)
    two_group = [two] + spread(two)
    state = attend(prompt_length, own, twin, own_group, None)
    state = attend(prompt_length, own, twin, one_group, state)
    state = attend(prompt_length, own, twin, other_group, state)
    state = attend(prompt_length, own, twin, two_group, state, last=True)
    got = move(state[2], dc=1)
    done = merge(state[0], state[1], got)
    parts = [done[0]] + [turn(done[d], -d) for d in range(1, BLOCK)]
    weight, done = lax.optimization_barrier((out_weight, done))
    weight = hold(weight)
    return project(member.reshape(1), positions, parts, weight, residual)


def solution(mesh):
    def step(*args):
        return on_device(mesh.shape["seq"], *args)

    return jax.shard_map(
        step,
        mesh=mesh,
        in_specs=(
            P(("groups", "seq"), None),
            P(("groups", "seq"), None),
            P(("groups", "seq"), None),
            P(("groups", "seq")),
            P("groups"),
            P(),
            P(("groups", "seq"), None),
        ),
        out_specs=P(("groups", "seq"), None),
        check_vma=False,
    )
```

```python
import functools
import math
import jax
import jax.numpy as jnp
from jax import lax
from jax.experimental import pallas as pl
from jax.experimental.pallas import tpu as pltpu
from jax.sharding import PartitionSpec as P

HEADS = 16
KV_HEADS = 4
HEAD_DIM = 128
GROUP = HEADS // KV_HEADS
TOK = 64
RUN = 128
X_DEV = 4
CORES = 2
BLOCK = KV_HEADS
HALF = 32
KV_ROWS = 2 * TOK + 8
ALL_ROWS = (2 + GROUP) * TOK + 8
TOGETHER = 2
ROWS = TOGETHER * GROUP * HALF
PAIRS = KV_HEADS // TOGETHER
SCALE = HEAD_DIM ** -0.5 * math.log2(math.e)
PART = 32
NEVER = -1e30
LOWEST = -1e20
VMEM = pltpu.VMEM
F32 = jnp.float32
BF16 = jnp.bfloat16


def iota(shape, dim):
    return lax.broadcasted_iota(jnp.int32, shape, dim)


def prep_kernel(pos_hbm, q_hbm, k_hbm, v_hbm, out_ref, pos_ref, q_ref, k_ref, v_ref, arrived):
    copies = [
        pltpu.make_async_copy(source, target, arrived.at[n])
        for n, (source, target) in enumerate(
            ((pos_hbm, pos_ref), (k_hbm, k_ref), (v_hbm, v_ref), (q_hbm, q_ref))
        )
    ]
    for copy in copies:
        copy.start()
    copies[0].wait()
    pos = pos_ref[...]
    run = pos // RUN
    off = (pos - run * RUN).astype(F32)
    pick = (iota((TOK, TOK), 0) == jnp.broadcast_to(run, (TOK, TOK))).astype(F32)
    pick16 = pick.astype(BF16)
    off_col = jnp.dot(
        (pick * jnp.broadcast_to(off, (TOK, TOK))).astype(BF16),
        jnp.ones((TOK, HEAD_DIM), BF16),
        preferred_element_type=F32,
    )
    row = iota((TOK, HEAD_DIM), 0)
    lane = iota((TOK, HEAD_DIM), 1)
    lines = [
        jnp.sum(jnp.where(row == HALF * j + lane % HALF, off_col, 0.0), axis=0, keepdims=True)
        for j in range(TOK // HALF)
    ]
    table = jnp.concatenate(lines + [jnp.zeros((8 - len(lines), HEAD_DIM), F32)], axis=0).astype(BF16)
    copies[1].wait()
    sorted_k = jnp.dot(pick16, k_ref[...], preferred_element_type=F32).astype(BF16)
    copies[2].wait()
    sorted_v = jnp.dot(pick16, v_ref[...], preferred_element_type=F32).astype(BF16)
    copies[3].wait()
    sorted_q = jnp.dot(pick16, q_ref[...], preferred_element_type=F32).astype(BF16)
    for h in range(KV_HEADS):
        cols = slice(h * HEAD_DIM, (h + 1) * HEAD_DIM)
        out_ref[h, 0:TOK, :] = sorted_k[:, cols]
        out_ref[h, TOK:2 * TOK, :] = sorted_v[:, cols]
        for g in range(GROUP):
            at = (h * GROUP + g) * HEAD_DIM
            out_ref[h, (2 + g) * TOK:(3 + g) * TOK, :] = sorted_q[:, at:at + HEAD_DIM]
        out_ref[h, (2 + GROUP) * TOK:ALL_ROWS, :] = table


def in_hbm(a):
    return pltpu.with_memory_space_constraint(a, pltpu.HBM)


def prep(positions, query_rows, key_rows, value_rows):
    return pl.pallas_call(
        prep_kernel,
        out_shape=VMEM((KV_HEADS, ALL_ROWS, HEAD_DIM), BF16),
        in_specs=[pl.BlockSpec(memory_space=pltpu.HBM)] * 4,
        out_specs=pl.BlockSpec(memory_space=VMEM),
        scratch_shapes=[
            VMEM((1, TOK), jnp.int32),
            VMEM(query_rows.shape, BF16),
            VMEM(key_rows.shape, BF16),
            VMEM(value_rows.shape, BF16),
            pltpu.SemaphoreType.DMA((4,)),
        ],
        compiler_params=pltpu.CompilerParams(vmem_limit_bytes=8 * 1024 * 1024),
        cost_estimate=pl.CostEstimate(flops=TOK * TOK * 3072 * 2, bytes_accessed=800_000, transcendentals=0),
        name="prep",
    )(*(in_hbm(a) for a in (positions.reshape(1, TOK), query_rows, key_rows, value_rows)))


def attend_kernel(parts, first, last, *refs):
    limit_ref, qa_ref, qb_ref = refs[:3]
    kv_refs = refs[3:3 + parts]
    refs = refs[3 + parts:]
    if first:
        old_refs = None
    else:
        offsets, old_refs, refs = refs[0], refs[1:5], refs[5:]
    new_refs, (keys, vals) = refs[:-2], refs[-2:]
    limit = limit_ref[0]
    sources = KV_HEADS
    units = [(kv, at) for kv in kv_refs for at in range(0, kv.shape[0], sources)]
    shards = len(units)
    wide = shards * HEAD_DIM
    for j in range(2):
        for n, (kv, base) in enumerate(units):
            for s in range(sources):
                at = j * wide + (n * sources + s) * HALF
                keys[at:at + HALF, :] = kv[base + s, HALF * j:HALF * (j + 1), :]
                vals[at:at + HALF, 0:HEAD_DIM] = kv[base + s, TOK + HALF * j:TOK + HALF * (j + 1), :]
    vals[:, HEAD_DIM:] = jnp.ones((2 * wide, HEAD_DIM), BF16)
    lane8 = iota((8, HEAD_DIM), 1)
    tables = []
    for kv, base in units:
        table = kv[base, 2 * TOK:KV_ROWS, :].astype(F32)
        for s in range(1, sources):
            table = jnp.where(lane8 // HALF == s, kv[base + s, 2 * TOK:KV_ROWS, :].astype(F32), table)
        table = table + (lane8 % HALF * RUN).astype(F32)
        chunk = (iota((8, HEAD_DIM), 0) * (HALF * RUN)).astype(F32)
        tables.append(jnp.where(table + chunk >= limit.astype(F32), 1e9, table))
    ramp = (iota((HALF, HEAD_DIM), 0) * RUN).astype(F32)
    if first:
        diagonal = iota((HALF, HEAD_DIM), 0) == iota((HALF, HEAD_DIM), 1)
        spread = [
            jnp.where(diagonal, q_ref[src, ALL_ROWS - 8 + i:ALL_ROWS - 7 + i, :].astype(F32), 0.0).astype(BF16)
            for q_ref in (qa_ref, qb_ref)
            for i in range(2)
            for src in range(sources)
        ]
        offsets = new_refs[4]
        offsets[...] = jnp.dot(
            jnp.concatenate(spread, axis=0), jnp.ones((HEAD_DIM, HEAD_DIM), BF16), preferred_element_type=F32
        )
    blocks = [(half, i, sp) for half in range(2) for i in range(2) for sp in range(PAIRS)]

    def score(half, i, sp):
        q_ref = (qa_ref, qb_ref)[half]
        q_rows = []
        for src in range(TOGETHER * sp, TOGETHER * (sp + 1)):
            for g in range(GROUP):
                at = (2 + g) * TOK + HALF * i
                q_rows.append(q_ref[src, at:at + HALF, :])
        return lax.dot_general(
            jnp.concatenate(q_rows, axis=0),
            keys[0:(i + 1) * wide, :],
            (((1,), (1,)), ((), ())),
            preferred_element_type=F32,
        )

    ready = score(*blocks[0])
    for at_block, (half, i, sp) in enumerate(blocks):
        s = ready * SCALE
        if at_block + 1 < len(blocks):
            ready = score(*blocks[at_block + 1])
        b = i * PAIRS + sp
        q_poss = []
        for src in range(TOGETHER * sp, TOGETHER * (sp + 1)):
            at = ((half * 2 + i) * sources + src) * HALF
            q_poss += [offsets[at:at + HALF, :] + ramp] * GROUP
        q_pos = jnp.concatenate(q_poss, axis=0)
        count = (i + 1) * wide
        pieces = [s[:, c * HEAD_DIM:(c + 1) * HEAD_DIM] for c in range(count // HEAD_DIM)]
        for n in range(shards):
            c = i * shards + n
            pieces[c] = jnp.where(tables[n][i:i + 1, :] <= q_pos, pieces[c], NEVER)
        top = functools.reduce(jnp.maximum, pieces)
        top = jnp.max(top, axis=1, keepdims=True)
        if first:
            new_max = jnp.broadcast_to(jnp.maximum(top, LOWEST), (ROWS, HEAD_DIM))
        else:
            old_max = old_refs[2 * half][b]
            new_max = jnp.maximum(old_max, top)
        weights = jnp.concatenate([jnp.exp2(piece - new_max).astype(BF16) for piece in pieces], axis=1)
        sums = jnp.dot(weights, vals[0:count, :], preferred_element_type=F32)
        if not first:
            rescale = jnp.exp2(old_max - new_max)
            sums = sums + old_refs[2 * half + 1][b] * jnp.concatenate([rescale, rescale], axis=1)
        if last and half == 1:
            lane = iota((ROWS, HEAD_DIM), 1)
            total = jnp.maximum(sums[:, HEAD_DIM:], 1e-30)
            level = new_max + jnp.log2(total)
            high = level.astype(BF16).astype(F32)
            middle = (level - high).astype(BF16).astype(F32)
            parts3 = jnp.where(lane < PART, high, jnp.where(lane < 2 * PART, middle, level - high - middle))
            new_refs[2][b, :, 0:HEAD_DIM] = (sums[:, 0:HEAD_DIM] / total).astype(BF16)
            new_refs[2][b, :, HEAD_DIM:] = parts3.astype(BF16)
        else:
            new_refs[2 * half][b] = new_max
            new_refs[2 * half + 1][b] = sums


def attend(limit, qa, qb, parts, state, offsets=None, last=False):
    shards = sum(part.shape[0] for part in parts) // KV_HEADS
    wide = shards * HEAD_DIM
    stats = jax.ShapeDtypeStruct((2 * PAIRS, ROWS, HEAD_DIM), F32)
    sums = jax.ShapeDtypeStruct((2 * PAIRS, ROWS, 2 * HEAD_DIM), F32)
    shapes = (stats, sums, VMEM(sums.shape, BF16)) if last else (stats, sums, stats, sums)
    first = state is None
    held = [] if first else [offsets] + list(state)
    if first:
        shapes += (jax.ShapeDtypeStruct((4 * KV_HEADS * HALF, HEAD_DIM), F32),)
    score_count = 4 * 2 * 256 * 3 * wide
    base = 4 + len(parts)
    return pl.pallas_call(
        functools.partial(attend_kernel, len(parts), first, last),
        out_shape=shapes,
        in_specs=[pl.BlockSpec(memory_space=pltpu.SMEM)] + [pl.BlockSpec(memory_space=VMEM)] * (2 + len(parts) + len(held)),
        out_specs=(pl.BlockSpec(memory_space=VMEM),) * len(shapes),
        scratch_shapes=[VMEM((2 * wide, HEAD_DIM), BF16), VMEM((2 * wide, 2 * HEAD_DIM), BF16)],
        input_output_aliases={} if first else ({base: 0, base + 1: 1} if last else {base + n: n for n in range(4)}),
        compiler_params=pltpu.CompilerParams(vmem_limit_bytes=12 * 1024 * 1024),
        cost_estimate=pl.CostEstimate(
            flops=score_count * HEAD_DIM * 6, bytes_accessed=4_000_000, transcendentals=score_count
        ),
        name="attend_last" if last else "attend",
    )(limit, qa, qb, *parts, *held)


def hold_kernel(weight_ref, held_ref, arrived):
    copy = pltpu.make_async_copy(weight_ref, held_ref, arrived)
    copy.start()
    copy.wait()


def hold(weight):
    return pl.pallas_call(
        hold_kernel,
        out_shape=VMEM(weight.shape, weight.dtype),
        in_specs=[pl.BlockSpec(memory_space=pltpu.HBM)],
        out_specs=pl.BlockSpec(memory_space=VMEM),
        scratch_shapes=[pltpu.SemaphoreType.DMA],
        compiler_params=pltpu.CompilerParams(vmem_limit_bytes=10 * 1024 * 1024),
        cost_estimate=pl.CostEstimate(flops=2_000_000_000, bytes_accessed=8_000_000, transcendentals=0),
        name="hold",
    )(in_hbm(weight))


def merge_kernel(max_ref, sum_ref, got_ref, out_ref):
    for i in range(2):
        for sp in range(PAIRS):
            b = i * PAIRS + sp
            max_a = max_ref[b]
            level = got_ref[b, :, HEAD_DIM:].astype(F32)
            level = level[:, 0:1] + level[:, PART:PART + 1] + level[:, 2 * PART:2 * PART + 1]
            max_b = jnp.broadcast_to(level, (ROWS, HEAD_DIM))
            top = jnp.maximum(max_a, max_b)
            part_a = jnp.exp2(max_a - top)
            part_b = jnp.exp2(max_b - top)
            total = sum_ref[b, :, HEAD_DIM:] * part_a + part_b
            value = sum_ref[b, :, 0:HEAD_DIM] * part_a + got_ref[b, :, 0:HEAD_DIM].astype(F32) * part_b
            value = (value / total).astype(BF16).reshape(TOGETHER, GROUP, HALF, HEAD_DIM)
            out_ref[TOGETHER * sp:TOGETHER * (sp + 1), :, HALF * i:HALF * (i + 1), :] = value


def merge(maxima, sums, got):
    return pl.pallas_call(
        merge_kernel,
        out_shape=jax.ShapeDtypeStruct((KV_HEADS, GROUP, TOK, HEAD_DIM), BF16),
        in_specs=[pl.BlockSpec(memory_space=VMEM)] * 3,
        out_specs=pl.BlockSpec(memory_space=VMEM),
        compiler_params=pltpu.CompilerParams(vmem_limit_bytes=12 * 1024 * 1024),
        cost_estimate=pl.CostEstimate(flops=4_000_000, bytes_accessed=3_000_000, transcendentals=300_000),
        name="merge",
    )(maxima, sums, got)


def project_kernel(member_ref, pos_ref, *refs):
    parts = refs[:KV_HEADS]
    weight_ref, residual_ref, out_ref, heads = refs[KV_HEADS:]
    member = member_ref[0]
    for d, part in enumerate(parts):
        heads[lax.rem(member + d, KV_HEADS)] = part[...]
    run = pos_ref[...] // RUN
    put = (jnp.broadcast_to(run, (TOK, TOK)) == iota((TOK, TOK), 1)).astype(F32).astype(BF16)
    rows = jnp.concatenate([heads[h, g] for h in range(KV_HEADS) for g in range(GROUP)], axis=1)
    rows = jnp.dot(put, rows, preferred_element_type=F32).astype(BF16)
    wide = 512
    for n in range(weight_ref.shape[1] // wide):
        cols = slice(n * wide, (n + 1) * wide)
        total = jnp.dot(rows, weight_ref[:, cols], preferred_element_type=F32)
        out_ref[:, cols] = (total + residual_ref[:, cols].astype(F32)).astype(BF16)


def project(member, positions, parts, out_weight, residual):
    return pl.pallas_call(
        project_kernel,
        out_shape=jax.ShapeDtypeStruct(residual.shape, BF16),
        in_specs=[pl.BlockSpec(memory_space=pltpu.SMEM)] + [pl.BlockSpec(memory_space=VMEM)] * (len(parts) + 3),
        out_specs=pl.BlockSpec(memory_space=VMEM),
        scratch_shapes=[VMEM((KV_HEADS, GROUP, TOK, HEAD_DIM), BF16)],
        compiler_params=pltpu.CompilerParams(vmem_limit_bytes=12 * 1024 * 1024),
        cost_estimate=pl.CostEstimate(flops=TOK * 2048 * 4096, bytes_accessed=9_000_000, transcendentals=0),
        name="project",
    )(member, positions.reshape(TOK, 1), *parts, out_weight, residual)


def on_device(seq_size, query_rows, key_rows, value_rows, positions, prompt_length, out_weight, residual):
    z_dev = seq_size // (X_DEV * CORES)

    def at(z, x, c):
        return ((z % z_dev) * X_DEV + x % X_DEV) * CORES + c % CORES

    spots = [(z, x, c) for z in range(z_dev) for x in range(X_DEV) for c in range(CORES)]

    def move(a, dz=0, dx=0, dc=0):
        return lax.ppermute(a, "seq", [(at(z, x, c), at(z + dz, x + dx, c + dc)) for z, x, c in spots])

    def far(a):
        return lax.ppermute(
            a, "seq", [(at(z, x, c), at(z + (BLOCK if c == 0 else -BLOCK), x, c)) for z, x, c in spots]
        )

    def turn(a, d):
        return lax.ppermute(
            a, "seq", [(at(z, x, c), at(z // BLOCK * BLOCK + (z + d) % BLOCK, x, c)) for z, x, c in spots]
        )

    def spread(a):
        return [move(a, dx=1), move(a, dx=-1), move(a, dx=2)]

    member = lax.rem(lax.axis_index("seq") // (X_DEV * CORES), BLOCK)
    message = prep(positions, query_rows, key_rows, value_rows)
    pick = [lax.dynamic_index_in_dim(message, lax.rem(member + d, BLOCK), 0, keepdims=False) for d in range(BLOCK)]
    own = jnp.stack([pick[0]] + [turn(pick[d], d) for d in range(1, BLOCK)])
    twin = move(own, dc=1)

    def kv_of(a):
        return jnp.concatenate([a[:, 0:2 * TOK], a[:, ALL_ROWS - 8:]], axis=1)

    mine = kv_of(own)
    one = far(mine)
    other = far(kv_of(twin))
    own_group = [mine] + spread(mine)
    two = far(one)
    one_group = [one] + spread(one)
    other_group = [other] + spread(other)
    two_group = [two] + spread(two)
    *state, offsets = attend(prompt_length, own, twin, own_group, None)
    state = attend(prompt_length, own, twin, one_group, state, offsets)
    state = attend(prompt_length, own, twin, other_group, state, offsets)
    state = attend(prompt_length, own, twin, two_group, state, offsets, last=True)
    got = move(state[2], dc=1)
    done = merge(state[0], state[1], got)
    parts = [done[0]] + [turn(done[d], -d) for d in range(1, BLOCK)]
    weight, done = lax.optimization_barrier((out_weight, done))
    weight = hold(weight)
    return project(member.reshape(1), positions, parts, weight, residual)


def solution(mesh):
    def step(*args):
        return on_device(mesh.shape["seq"], *args)

    return jax.shard_map(
        step,
        mesh=mesh,
        in_specs=(
            P(("groups", "seq"), None),
            P(("groups", "seq"), None),
            P(("groups", "seq"), None),
            P(("groups", "seq")),
            P("groups"),
            P(),
            P(("groups", "seq"), None),
        ),
        out_specs=P(("groups", "seq"), None),
        check_vma=False,
    )
```
